256 devices in a mesh: rep: 64 (over z, y, x_hi), seq: 4 (over x_lo, core).
Axes of the slice: x: 4 (x_hi: 2, x_lo: 2; x = x_hi * 2 + x_lo), y: 4, z: 8, core: 2. Of those that a mesh axis runs over, the one named last changes fastest.
Arguments:
- inputs: bfloat16 [64, 2048, 2048], P('rep', 'seq'), may hold values from -6 to 6
- query: bfloat16 [64, 2048, 1024], P('rep', 'seq'), may hold values from -6 to 6
- key_feat: bfloat16 [64, 2048, 1024], P('rep', 'seq'), may hold values from -6 to 6
- cotangent: bfloat16 [64, 2048, 2048], P('rep', 'seq'), may hold values from -6 to 6
- value_weight: bfloat16 [64, 2048, 1024], P('rep', 'seq'), may hold values from -6 to 6
- output_weight: bfloat16 [64, 1024, 2048], P('rep', 'seq'), may hold values from -6 to 6
- stale_value: bfloat16 [64, 2048, 1024], P('rep', 'seq'), may hold values from -6 to 6
- stale_output: bfloat16 [64, 1024, 2048], P('rep', 'seq'), may hold values from -6 to 6
- step_counts: int32 [64], replicated, may hold values from 1 to 999
- partner: int32 [64], replicated, may hold values from 0 to 63, as said below
Outputs:
- new_value: bfloat16 [64, 2048, 1024], P('rep', 'seq')
- new_output: bfloat16 [64, 1024, 2048], P('rep', 'seq')
The draws below stay inside these ranges and needn't reach their ends.
Inputs may be any that keep to these rules, and one draw needn't show every extreme that they name: partner pairs the replicas: partner[partner[r]] = r and partner[r] != r for every r.
All inputs are finite; a program needn't handle non-finite values.
Results may differ from the reference program's by a relative error of at most 0.009.
Values may be sent and summed in bfloat16 or wider, within the bound.
No kernel may reach another device: no remote copies, remote signals or barrier semaphores. Data moves between devices by JAX's collectives and lax.ppermute only.
A program may use at most 128 MiB of HBM per device.

```python
import jax
import jax.numpy as jnp
from jax import lax

D = 2048
HEADS = 16
HEAD = 64
TOK_DEV = 512
HD = 1024
TOKENS = 2048
REPS = 64
N_SEQ = 4


def draw_partner(key, part):
    order = jax.random.permutation(jax.random.fold_in(key, 7), REPS).astype(jnp.int32)
    paired = order.reshape(REPS // 2, 2)[:, ::-1].reshape(REPS)
    return jnp.zeros((REPS,), jnp.int32).at[order].set(paired)


def place_ends(drawn, key, least, high):
    dims = drawn.shape
    spot = [jax.random.randint(jax.random.fold_in(key, axis), (), 0, dims[axis]) for axis in range(len(dims))]
    drawn = drawn.at[tuple(spot)].set(least)
    longest = dims.index(max(dims))
    spot[longest] = (spot[longest] + 1) % dims[longest]
    return drawn.at[tuple(spot)].set(high)


def block_scale(own_key, extent, cuts, least, top_value):
    loudness, own = 1.0, jax.random.fold_in(own_key, 6)
    for position, blocks in cuts:
        draws = jnp.exp(jax.random.uniform(jax.random.fold_in(own, position), (blocks,), jnp.float32, least / len(cuts), top_value / len(cuts)))
        loudness = loudness * jnp.repeat(draws, extent[position] // blocks).reshape([-1 if axis == position else 1 for axis in range(len(extent))])
    return loudness


def scatter_about(rng, dims, deviation, most, pieces=(), kind=jnp.bfloat16):
    values = deviation * jax.random.normal(rng, dims, jnp.float32)
    if pieces:
        values = values * block_scale(rng, dims, pieces, -0.22, 0.18)
    return jnp.clip(values, -most, most).astype(kind)


def setup_inputs(seed: int = 0) -> dict:
    keys = jax.random.split(jax.random.key(seed), 11)
    inputs = scatter_about(keys[0], (REPS, TOKENS, D), 1.0, 6.0, ((0, 64), (1, 4)))
    query = scatter_about(keys[1], (REPS, TOKENS, HD), 1.0, 6.0, ((0, 64), (1, 4)))
    key_feat = scatter_about(keys[2], (REPS, TOKENS, HD), 1.0, 6.0, ((0, 64), (1, 4)))
    cotangent = scatter_about(keys[3], (REPS, TOKENS, D), 1.0, 6.0, ((0, 64), (1, 4)))
    value_weight = scatter_about(keys[4], (REPS, D, HD), 1.0, 6.0, ((0, 64), (1, 4)))
    output_weight = scatter_about(keys[5], (REPS, HD, D), 1.0, 6.0, ((0, 64), (1, 4)))
    stale_value = scatter_about(keys[6], (REPS, D, HD), 1.0, 6.0, ((0, 64), (1, 4)))
    stale_output = scatter_about(keys[7], (REPS, HD, D), 1.0, 6.0, ((0, 64), (1, 4)))
    step_counts = place_ends(jax.random.randint(keys[8], (REPS,), 1, 1000), jax.random.fold_in(keys[8], 1), 1, 999).astype(jnp.int32)
    partner = draw_partner(jax.random.fold_in(keys[10], 71), 0)
    return {"inputs": inputs, "query": query, "key_feat": key_feat, "cotangent": cotangent, "value_weight": value_weight, "output_weight": output_weight, "stale_value": stale_value, "stale_output": stale_output, "step_counts": step_counts, "partner": partner}


learning_rate = 0.25
norm_eps = 1e-06

def rounded(array):
    return lax.optimization_barrier(array.astype(jnp.bfloat16)).astype(jnp.float32)

def reference(inputs, query, key_feat, cotangent, value_weight, output_weight, stale_value, stale_output, step_counts, partner):
    width = HEADS * HEAD
    scale_value = D ** (-0.5)
    scale_output = width ** (-0.5)
    highest = lax.Precision.HIGHEST
    causal = jnp.arange(TOK_DEV)[:, None] >= jnp.arange(TOK_DEV)[None, :]

    def replica(index):
        mate = partner[index]
        features = inputs[index]
        weight_v = value_weight[index]
        weight_o = output_weight[index]
        upstream_rows = cotangent[index]
        values = rounded(jnp.dot(features, weight_v, preferred_element_type=jnp.float32) * scale_value)
        query_blocks = query[index].astype(jnp.float32).reshape(N_SEQ, TOK_DEV, HEADS, HEAD)
        key_blocks = key_feat[index].astype(jnp.float32).reshape(N_SEQ, TOK_DEV, HEADS, HEAD)
        value_blocks = values.reshape(N_SEQ, TOK_DEV, HEADS, HEAD)
        states = jnp.einsum('bthe,bthf->bhef', key_blocks, value_blocks, precision=highest)
        running = jnp.cumsum(states, axis=0)
        prior = rounded(jnp.concatenate([jnp.zeros_like(states[:1]), running[:-1]], axis=0))
        scores = jnp.einsum('bthe,bshe->bhts', query_blocks, key_blocks, precision=highest)
        scores = rounded(jnp.where(causal, scores, jnp.float32(0.0)))
        attn = jnp.einsum('bhts,bshf->bthf', scores, value_blocks, precision=highest)
        attn = attn + jnp.einsum('bthe,bhef->bthf', query_blocks, prior, precision=highest)
        inverse = lax.rsqrt(lax.optimization_barrier(jnp.mean(attn * attn, axis=-1, keepdims=True)) + norm_eps)
        unit = attn * inverse
        normed = rounded(unit)
        upstream = jnp.dot(upstream_rows, weight_o.T, preferred_element_type=jnp.float32) * scale_output
        upstream = upstream.reshape(N_SEQ, TOK_DEV, HEADS, HEAD)
        d_attn = rounded(inverse * (upstream - unit * lax.optimization_barrier(jnp.mean(unit * upstream, axis=-1, keepdims=True))))
        grad_states = jnp.einsum('bthe,bthf->bhef', query_blocks, d_attn, precision=highest)
        backward = jnp.cumsum(grad_states[::-1], axis=0)[::-1]
        later = rounded(jnp.concatenate([backward[1:], jnp.zeros_like(grad_states[:1])], axis=0))
        d_values = jnp.einsum('bhts,bthf->bshf', scores, d_attn, precision=highest)
        d_values = rounded(d_values + jnp.einsum('bshe,bhef->bshf', key_blocks, later, precision=highest))
        d_values = d_values.reshape(N_SEQ, TOK_DEV, width)
        feature_blocks = features.astype(jnp.float32).reshape(N_SEQ, TOK_DEV, D)
        grad_value = lax.optimization_barrier(jnp.sum(rounded(jnp.einsum('btd,btf->bdf', feature_blocks, d_values, precision=highest) * scale_value), axis=0))
        normed_blocks = normed.reshape(N_SEQ, TOK_DEV, width)
        upstream_blocks = upstream_rows.astype(jnp.float32).reshape(N_SEQ, TOK_DEV, D)
        grad_output = lax.optimization_barrier(jnp.sum(rounded(jnp.einsum('btf,btd->bfd', normed_blocks, upstream_blocks, precision=highest) * scale_output), axis=0))
        own_count = step_counts[index].astype(jnp.float32)
        mate_count = step_counts[mate].astype(jnp.float32)
        mix = mate_count / (own_count + mate_count)
        new_value = (1.0 - mix) * weight_v.astype(jnp.float32) + mix * stale_value[mate].astype(jnp.float32) - learning_rate * grad_value
        new_output = (1.0 - mix) * weight_o.astype(jnp.float32) + mix * stale_output[mate].astype(jnp.float32) - learning_rate * grad_output
        return (new_value.astype(jnp.bfloat16), new_output.astype(jnp.bfloat16))
    new_value, new_output = lax.map(replica, jnp.arange(REPS, dtype=jnp.int32))
    return (new_value, new_output)
```

```python
import jax
import jax.numpy as jnp
from jax import lax
from jax.sharding import PartitionSpec as P

D = 2048
HEADS = 16
HEAD = 64

learning_rate = 0.25
norm_eps = 1e-06

ACROSS = [(0, 2), (2, 0), (1, 3), (3, 1)]
TWIN = [(0, 1), (1, 0), (2, 3), (3, 2)]
f32 = jnp.float32
bf16 = jnp.bfloat16


def sent(x, pairs):
    return lax.ppermute(x, "seq", pairs)


def column_block(x, block, width):
    return lax.dynamic_slice(x, (0, block * width), (x.shape[0], width))


def state_sums(states, order):
    total = None
    for step in order:
        piece = sent(states, step).astype(f32)
        total = piece if total is None else total + piece
    return total.astype(bf16)


BEFORE = ([(0, 1), (2, 3)], [(0, 2), (1, 3)], [(0, 3), (1, 2)])
AFTER = ([(1, 0), (3, 2)], [(2, 0), (3, 1)], [(3, 0), (2, 1)])


def pieces_of(value, output, count):
    rows = value.shape[0] // count
    width = value.shape[1]
    value = value.reshape(count, rows, width)
    output = output.reshape(count // 2, rows, 2, width).transpose(0, 2, 1, 3)
    return value, output.reshape(count, rows, width)


def fetch_partner(stale_value, stale_output, partner):
    count = lax.axis_size("rep")
    value, output = pieces_of(stale_value, stale_output, count)

    def swap(x):
        return lax.all_to_all(x, "rep", split_axis=0, concat_axis=0, tiled=True)

    def pick(x):
        return x.at[partner].get(mode="promise_in_bounds", unique_indices=True)

    value, output = swap(value), swap(output)
    value, output = swap(pick(value)), swap(pick(output))
    rows, width = value.shape[1:]
    output = output.reshape(count // 2, 2, rows, width).transpose(0, 2, 1, 3)
    return value.reshape(stale_value.shape), output.reshape(stale_output.shape)


def on_device(
    inputs, query, key_feat, cotangent, value_weight, output_weight,
    stale_value, stale_output, step_counts, partner,
):
    features = inputs[0]
    upstream_rows = cotangent[0]
    weight_v = value_weight[0]
    weight_o = output_weight[0]
    positions = features.shape[0]
    width = weight_v.shape[1]
    scale_value = D ** (-0.5)
    scale_output = width ** (-0.5)
    rank = lax.axis_index("seq")
    core = rank % 2
    rows_v = weight_v.shape[0]
    rows_o = weight_o.shape[0]

    across_v = sent(weight_v, ACROSS)
    twin_v = sent(weight_v, TWIN)
    both_v = sent(across_v, TWIN)
    across_o = sent(weight_o, ACROSS)
    twin_o = sent(weight_o, TWIN)
    both_o = sent(across_o, TWIN)
    mate_value, mate_output = fetch_partner(stale_value[0], stale_output[0], partner)

    twin_features = sent(
        jnp.concatenate(
            [column_block(features, 1 - core, rows_v), column_block(features, 3 - core, rows_v)],
            axis=1,
        ),
        TWIN,
    )
    twin_rows = sent(upstream_rows, TWIN)

    values = None
    for step, block in ((0, weight_v), (1, twin_v), (2, across_v), (3, both_v)):
        part = jnp.dot(
            column_block(features, rank ^ step, rows_v), block, preferred_element_type=f32
        )
        values = part if values is None else values + part
    values = (values * scale_value).astype(bf16)
    query_heads = query[0].reshape(positions, HEADS, HEAD)
    key_heads = key_feat[0].reshape(positions, HEADS, HEAD)
    value_heads = values.reshape(positions, HEADS, HEAD)
    states = jnp.einsum("the,thf->hef", key_heads, value_heads, preferred_element_type=f32)
    prior = state_sums(states.astype(bf16), BEFORE)
    causal = jnp.arange(positions)[:, None] >= jnp.arange(positions)[None, :]
    scores = jnp.einsum("the,she->hts", query_heads, key_heads, preferred_element_type=f32)
    scores = jnp.where(causal[None], scores, f32(0.0)).astype(bf16)
    attn = jnp.einsum("hts,shf->thf", scores, value_heads, preferred_element_type=f32)
    attn = attn + jnp.einsum("the,hef->thf", query_heads, prior, preferred_element_type=f32)
    inverse = lax.rsqrt(jnp.mean(attn * attn, axis=-1, keepdims=True) + norm_eps)
    unit = attn * inverse
    normed = unit.astype(bf16).reshape(positions, width)

    upstream = jnp.zeros((positions, width), f32)
    for step, block in ((0, weight_o), (1, twin_o), (2, across_o), (3, both_o)):
        part = lax.dot_general(
            upstream_rows, block, (((1,), (1,)), ((), ())), preferred_element_type=f32
        )
        upstream = lax.dynamic_update_slice(upstream, part, (0, (rank ^ step) * rows_o))
    upstream = (upstream * scale_output).reshape(positions, HEADS, HEAD)
    d_attn = inverse * (upstream - unit * jnp.mean(unit * upstream, axis=-1, keepdims=True))
    d_attn = d_attn.astype(bf16)
    grad_states = jnp.einsum("the,thf->hef", query_heads, d_attn, preferred_element_type=f32)
    later = state_sums(grad_states.astype(bf16), AFTER)
    d_values = jnp.einsum("hts,thf->shf", scores, d_attn, preferred_element_type=f32)
    d_values = d_values + jnp.einsum("she,hef->shf", key_heads, later, preferred_element_type=f32)
    d_values = d_values.astype(bf16).reshape(positions, width)

    twin_normed = sent(
        jnp.concatenate(
            [column_block(normed, 1 - core, rows_o), column_block(normed, 3 - core, rows_o)],
            axis=1,
        ),
        TWIN,
    )

    def rows_grad(mine, right, twin, twin_right, width, scale):
        def term(block):
            left = column_block(mine, block, width)
            other = column_block(twin, block // 2, width)
            dims = (((0,), (0,)), ((), ()))
            both = lax.dot_general(left, right, dims, preferred_element_type=f32)
            both += lax.dot_general(other, twin_right, dims, preferred_element_type=f32)
            return both * scale

        away = sent(term(rank ^ 2).astype(bf16), ACROSS)
        return term(rank) + away.astype(f32)

    grad_output = rows_grad(
        normed, upstream_rows, twin_normed, twin_rows, rows_o, scale_output
    )
    grad_value = rows_grad(
        features, d_values, twin_features, sent(d_values, TWIN), rows_v, scale_value
    )
    replica = lax.axis_index("rep")
    own_count = step_counts[replica].astype(f32)
    mate_count = step_counts[partner[replica]].astype(f32)
    mix = mate_count / (own_count + mate_count)
    new_value = (
        (1.0 - mix) * weight_v.astype(f32)
        + mix * mate_value.astype(f32)
        - learning_rate * grad_value
    )
    new_output = (
        (1.0 - mix) * weight_o.astype(f32)
        + mix * mate_output.astype(f32)
        - learning_rate * grad_output
    )
    return (new_value.astype(bf16)[None], new_output.astype(bf16)[None])


def solution(mesh):
    placed = (P("rep", "seq", None),) * 8 + (P(), P())
    return jax.shard_map(
        on_device,
        mesh=mesh,
        in_specs=placed,
        out_specs=(P("rep", "seq", None), P("rep", "seq", None)),
        check_vma=False,
    )
```

```python
import jax
import jax.numpy as jnp
from jax import lax
from jax.sharding import PartitionSpec as P


D = 2048
HEADS = 16
HEAD = 64

learning_rate = 0.25
norm_eps = 1e-06

ACROSS = [(0, 2), (2, 0), (1, 3), (3, 1)]
TWIN = [(0, 1), (1, 0), (2, 3), (3, 2)]
f32 = jnp.float32
bf16 = jnp.bfloat16


def sent(x, pairs):
    return lax.ppermute(x, "seq", pairs)


def column_block(x, block, width):
    return lax.dynamic_slice(x, (0, block * width), (x.shape[0], width))


def state_sums(states, order):
    total = None
    for step in order:
        piece = sent(states, step)
        total = piece.astype(f32) if total is None else total + piece.astype(f32)
    return total.astype(bf16)


BEFORE = ([(0, 1), (2, 3)], [(0, 2), (1, 3)], [(0, 3), (1, 2)])
AFTER = ([(1, 0), (3, 2)], [(2, 0), (3, 1)], [(3, 0), (2, 1)])


def after(x, *others):
    return lax.optimization_barrier((x, *others))[0]


def swap(x):
    return lax.all_to_all(x, "rep", split_axis=0, concat_axis=0, tiled=True)


def packed_pieces(value, output, count):
    rows = value.shape[0] // count
    width = value.shape[1]
    value = value.reshape(count, rows, width)
    output = output.reshape(count // 2, rows, 2, width).transpose(0, 2, 1, 3)
    return jnp.concatenate([value, output.reshape(count, rows, width)], axis=1)


def unpacked(pieces, value_shape, output_shape):
    count, rows, width = pieces.shape
    rows //= 2
    value = pieces[:, :rows].reshape(value_shape)
    output = pieces[:, rows:].reshape(count // 2, 2, rows, width).transpose(0, 2, 1, 3)
    return value, output.reshape(output_shape)


def on_device(
    inputs, query, key_feat, cotangent, value_weight, output_weight,
    stale_value, stale_output, step_counts, partner,
):
    features = inputs[0]
    upstream_rows = cotangent[0]
    weight_v = value_weight[0]
    weight_o = output_weight[0]
    positions = features.shape[0]
    width = weight_v.shape[1]
    scale_value = D ** (-0.5)
    scale_output = width ** (-0.5)
    rank = lax.axis_index("seq")
    core = rank % 2
    rows_v = weight_v.shape[0]
    rows_o = weight_o.shape[0]

    replicas = lax.axis_size("rep")
    across_v = sent(weight_v, ACROSS)
    twin_v = sent(weight_v, TWIN)
    both_v = sent(across_v, TWIN)
    spread = swap(packed_pieces(stale_value[0], stale_output[0], replicas))

    twin_features = sent(
        jnp.concatenate(
            [column_block(features, 1 - core, rows_v), column_block(features, 3 - core, rows_v)],
            axis=1,
        ),
        TWIN,
    )
    twin_rows = sent(upstream_rows, TWIN)

    values = None
    for step, block in ((0, weight_v), (1, twin_v), (2, across_v), (3, both_v)):
        part = jnp.dot(
            column_block(features, rank ^ step, rows_v), block, preferred_element_type=f32
        )
        values = part if values is None else values + part
    values = (values * scale_value).astype(bf16)
    query_heads = query[0].reshape(positions, HEADS, HEAD)
    key_heads = key_feat[0].reshape(positions, HEADS, HEAD)
    value_heads = values.reshape(positions, HEADS, HEAD)
    states = jnp.einsum("the,thf->hef", key_heads, value_heads, preferred_element_type=f32)
    states = states.astype(bf16)
    prior = state_sums(states, BEFORE)
    across_o = sent(after(weight_o, states), ACROSS)
    twin_o = sent(weight_o, TWIN)
    both_o = sent(across_o, TWIN)
    causal = jnp.arange(positions)[:, None] >= jnp.arange(positions)[None, :]
    scores = jnp.einsum("the,she->hts", query_heads, key_heads, preferred_element_type=f32)
    scores = jnp.where(causal[None], scores, f32(0.0)).astype(bf16)
    attn = jnp.einsum("hts,shf->thf", scores, value_heads, preferred_element_type=f32)
    attn = attn + jnp.einsum("the,hef->thf", query_heads, prior, preferred_element_type=f32)
    inverse = lax.rsqrt(jnp.mean(attn * attn, axis=-1, keepdims=True) + norm_eps)
    unit = attn * inverse
    normed = unit.astype(bf16).reshape(positions, width)

    upstream = jnp.zeros((positions, width), f32)
    for step, block in ((0, weight_o), (1, twin_o), (2, across_o), (3, both_o)):
        part = lax.dot_general(
            upstream_rows, block, (((1,), (1,)), ((), ())), preferred_element_type=f32
        )
        upstream = lax.dynamic_update_slice(upstream, part, (0, (rank ^ step) * rows_o))
    upstream = (upstream * scale_output).reshape(positions, HEADS, HEAD)
    d_attn = inverse * (upstream - unit * jnp.mean(unit * upstream, axis=-1, keepdims=True))
    d_attn = d_attn.astype(bf16)
    grad_states = jnp.einsum("the,thf->hef", query_heads, d_attn, preferred_element_type=f32)
    grad_states = grad_states.astype(bf16)
    later = state_sums(grad_states, AFTER)
    d_values = jnp.einsum("hts,thf->shf", scores, d_attn, preferred_element_type=f32)
    d_values = d_values + jnp.einsum("she,hef->shf", key_heads, later, preferred_element_type=f32)
    d_values = d_values.astype(bf16).reshape(positions, width)

    def rows_grad(mine, right, twin, twin_right, width, scale):
        def term(block):
            left = column_block(mine, block, width)
            other = column_block(twin, block // 2, width)
            dims = (((0,), (0,)), ((), ()))
            both = lax.dot_general(left, right, dims, preferred_element_type=f32)
            both += lax.dot_general(other, twin_right, dims, preferred_element_type=f32)
            return both * scale

        away = term(rank ^ 2).astype(bf16)
        back = sent(away, ACROSS)
        return away, back, term(rank)

    twin_normed = sent(
        jnp.concatenate(
            [column_block(normed, 1 - core, rows_o), column_block(normed, 3 - core, rows_o)],
            axis=1,
        ),
        TWIN,
    )
    away_o, back_o, own_o = rows_grad(
        normed, upstream_rows, twin_normed, twin_rows, rows_o, scale_output
    )
    grad_output = own_o + back_o.astype(f32)
    picked = after(spread, grad_states, away_o).at[partner].get(
        mode="promise_in_bounds", unique_indices=True
    )
    mate_value, mate_output = unpacked(swap(picked), weight_v.shape, weight_o.shape)
    _, back_v, own_v = rows_grad(
        features, d_values, twin_features, sent(d_values, TWIN), rows_v, scale_value
    )
    grad_value = own_v + back_v.astype(f32)
    replica = lax.axis_index("rep")
    own_count = step_counts[replica].astype(f32)
    mate_count = step_counts[partner[replica]].astype(f32)
    mix = mate_count / (own_count + mate_count)
    new_value = (
        (1.0 - mix) * weight_v.astype(f32)
        + mix * mate_value.astype(f32)
        - learning_rate * grad_value
    )
    new_output = (
        (1.0 - mix) * weight_o.astype(f32)
        + mix * mate_output.astype(f32)
        - learning_rate * grad_output
    )
    return (new_value.astype(bf16)[None], new_output.astype(bf16)[None])


def solution(mesh):
    placed = (P("rep", "seq", None),) * 8 + (P(), P())

    return jax.shard_map(
        on_device,
        mesh=mesh,
        in_specs=placed,
        out_specs=(P("rep", "seq", None), P("rep", "seq", None)),
        check_vma=False,
    )
```

```python
import jax
import jax.numpy as jnp
from jax import lax
from jax.sharding import PartitionSpec as P


D = 2048
HEADS = 16
HEAD = 64

learning_rate = 0.25
norm_eps = 1e-06

ACROSS = [(0, 2), (2, 0), (1, 3), (3, 1)]
TWIN = [(0, 1), (1, 0), (2, 3), (3, 2)]
f32 = jnp.float32
bf16 = jnp.bfloat16


def sent(x, pairs):
    return lax.ppermute(x, "seq", pairs)


def column_block(x, block, width):
    return lax.dynamic_slice(x, (0, block * width), (x.shape[0], width))


def state_sums(states, order):
    total = None
    for step in order:
        piece = sent(states, step)
        total = piece.astype(f32) if total is None else total + piece.astype(f32)
    return total.astype(bf16)


BEFORE = ([(0, 1), (2, 3)], [(0, 2), (1, 3)], [(0, 3), (1, 2)])
AFTER = ([(1, 0), (3, 2)], [(2, 0), (3, 1)], [(3, 0), (2, 1)])


def after(x, *others):
    return lax.optimization_barrier((x, *others))[0]


def swap(x):
    return lax.all_to_all(x, "rep", split_axis=0, concat_axis=0, tiled=True)


def value_pieces(x, count):
    return x.reshape(count, x.shape[0] // count, x.shape[1])


def output_pieces(x, count):
    rows, width = 2 * x.shape[0] // count, x.shape[1] // 2
    x = x.reshape(count // 2, rows, 2, width).transpose(0, 2, 1, 3)
    return x.reshape(count, rows, width)


def output_rows(pieces):
    count, rows, width = pieces.shape
    x = pieces.reshape(count // 2, 2, rows, width).transpose(0, 2, 1, 3)
    return x.reshape(count * rows // 2, 2 * width)


def on_device(
    inputs, query, key_feat, cotangent, value_weight, output_weight,
    stale_value, stale_output, step_counts, partner,
):
    features = inputs[0]
    upstream_rows = cotangent[0]
    weight_v = value_weight[0]
    weight_o = output_weight[0]
    positions = features.shape[0]
    width = weight_v.shape[1]
    scale_value = D ** (-0.5)
    scale_output = width ** (-0.5)
    rank = lax.axis_index("seq")
    core = rank % 2
    rows_v = weight_v.shape[0]
    rows_o = weight_o.shape[0]

    replicas = lax.axis_size("rep")
    across_v = sent(weight_v, ACROSS)
    twin_v = sent(weight_v, TWIN)
    both_v = sent(across_v, TWIN)
    published = [value_pieces(stale_value[0], replicas), output_pieces(stale_output[0], replicas)]
    spread = swap(jnp.concatenate(published, axis=1))

    twin_features = sent(
        jnp.concatenate(
            [column_block(features, 1 - core, rows_v), column_block(features, 3 - core, rows_v)],
            axis=1,
        ),
        TWIN,
    )
    twin_rows = sent(upstream_rows, TWIN)

    values = None
    for step, block in ((0, weight_v), (1, twin_v), (2, across_v), (3, both_v)):
        part = jnp.dot(
            column_block(features, rank ^ step, rows_v), block, preferred_element_type=f32
        )
        values = part if values is None else values + part
    values = (values * scale_value).astype(bf16)
    query_heads = query[0].reshape(positions, HEADS, HEAD)
    key_heads = key_feat[0].reshape(positions, HEADS, HEAD)
    value_heads = values.reshape(positions, HEADS, HEAD)
    states = jnp.einsum("the,thf->hef", key_heads, value_heads, preferred_element_type=f32)
    states = states.astype(bf16)
    prior = state_sums(states, BEFORE)
    across_o = sent(weight_o, ACROSS)
    twin_o = sent(weight_o, TWIN)
    both_o = sent(across_o, TWIN)
    causal = jnp.arange(positions)[:, None] >= jnp.arange(positions)[None, :]
    scores = jnp.einsum("the,she->hts", query_heads, key_heads, preferred_element_type=f32)
    scores = jnp.where(causal[None], scores, f32(0.0)).astype(bf16)
    attn = jnp.einsum("hts,shf->thf", scores, value_heads, preferred_element_type=f32)
    attn = attn + jnp.einsum("the,hef->thf", query_heads, prior, preferred_element_type=f32)
    inverse = lax.rsqrt(jnp.mean(attn * attn, axis=-1, keepdims=True) + norm_eps)
    unit = attn * inverse
    normed = unit.astype(bf16).reshape(positions, width)

    upstream = jnp.zeros((positions, width), f32)
    for step, block in ((0, weight_o), (1, twin_o), (2, across_o), (3, both_o)):
        part = lax.dot_general(
            upstream_rows, block, (((1,), (1,)), ((), ())), preferred_element_type=f32
        )
        upstream = lax.dynamic_update_slice(upstream, part, (0, (rank ^ step) * rows_o))
    upstream = (upstream * scale_output).reshape(positions, HEADS, HEAD)
    d_attn = inverse * (upstream - unit * jnp.mean(unit * upstream, axis=-1, keepdims=True))
    d_attn = d_attn.astype(bf16)
    grad_states = jnp.einsum("the,thf->hef", query_heads, d_attn, preferred_element_type=f32)
    grad_states = grad_states.astype(bf16)
    later = state_sums(grad_states, AFTER)
    d_values = jnp.einsum("hts,thf->shf", scores, d_attn, preferred_element_type=f32)
    d_values = d_values + jnp.einsum("she,hef->shf", key_heads, later, preferred_element_type=f32)
    d_values = d_values.astype(bf16).reshape(positions, width)

    def rows_grad(mine, right, twin, twin_right, width, scale):
        def term(block):
            left = column_block(mine, block, width)
            other = column_block(twin, block // 2, width)
            dims = (((0,), (0,)), ((), ()))
            both = lax.dot_general(left, right, dims, preferred_element_type=f32)
            both += lax.dot_general(other, twin_right, dims, preferred_element_type=f32)
            return both * scale

        away = term(rank ^ 2).astype(bf16)
        back = sent(away, ACROSS)
        return away, back, term(rank)

    twin_normed = sent(
        jnp.concatenate(
            [column_block(normed, 1 - core, rows_o), column_block(normed, 3 - core, rows_o)],
            axis=1,
        ),
        TWIN,
    )
    away_o, back_o, own_o = rows_grad(
        normed, upstream_rows, twin_normed, twin_rows, rows_o, scale_output
    )
    grad_output = own_o + back_o.astype(f32)
    picked = after(spread, grad_states, away_o).at[partner].get(
        mode="promise_in_bounds", unique_indices=True
    )
    fetched = swap(picked)
    _, back_v, own_v = rows_grad(
        features, d_values, twin_features, sent(d_values, TWIN), rows_v, scale_value
    )
    grad_value = own_v + back_v.astype(f32)
    replica = lax.axis_index("rep")
    own_count = step_counts[replica].astype(f32)
    mate_count = step_counts[partner[replica]].astype(f32)
    mix = mate_count / (own_count + mate_count)
    kept_value = (1.0 - mix) * weight_v.astype(f32) - learning_rate * grad_value
    kept_output = (1.0 - mix) * weight_o.astype(f32) - learning_rate * grad_output
    kept_value, kept_output = lax.optimization_barrier(
        (value_pieces(kept_value, replicas), output_pieces(kept_output, replicas))
    )
    half = kept_value.shape[1]
    new_value = (kept_value + mix * fetched[:, :half].astype(f32)).astype(bf16)
    new_output = (kept_output + mix * fetched[:, half:].astype(f32)).astype(bf16)
    return new_value.reshape(value_weight.shape), output_rows(new_output)[None]


def solution(mesh):
    placed = (P("rep", "seq", None),) * 8 + (P(), P())

    return jax.shard_map(
        on_device,
        mesh=mesh,
        in_specs=placed,
        out_specs=(P("rep", "seq", None), P("rep", "seq", None)),
        check_vma=False,
    )
```

```python
import jax
import jax.numpy as jnp
from jax import lax
from jax.sharding import PartitionSpec as P


D = 2048
HEADS = 16
HEAD = 64

learning_rate = 0.25
norm_eps = 1e-06


ACROSS = [(0, 2), (2, 0), (1, 3), (3, 1)]
TWIN = [(0, 1), (1, 0), (2, 3), (3, 2)]
f32 = jnp.float32
bf16 = jnp.bfloat16


def sent(x, pairs):
    return lax.ppermute(x, "seq", pairs)


def column_block(x, block, width):
    return lax.dynamic_slice(x, (0, block * width), (x.shape[0], width))


def state_sums(states, order):
    total = None
    for step in order:
        piece = sent(states, step)
        total = piece.astype(f32) if total is None else total + piece.astype(f32)
    return total.astype(bf16)


BEFORE = ([(0, 1), (2, 3)], [(0, 2), (1, 3)], [(0, 3), (1, 2)])
AFTER = ([(1, 0), (3, 2)], [(2, 0), (3, 1)], [(3, 0), (2, 1)])


def after(x, *others):
    return lax.optimization_barrier((x, *others))[0]


def swap(x):
    return lax.all_to_all(x, "rep", split_axis=0, concat_axis=0, tiled=True)


def value_pieces(x, count):
    return x.reshape(count, x.shape[0] // count, x.shape[1])


def output_pieces(x, count):
    rows, width = 2 * x.shape[0] // count, x.shape[1] // 2
    x = x.reshape(count // 2, rows, 2, width).transpose(0, 2, 1, 3)
    return x.reshape(count, rows, width)


def output_rows(pieces):
    count, rows, width = pieces.shape
    x = pieces.reshape(count // 2, 2, rows, width).transpose(0, 2, 1, 3)
    return x.reshape(count * rows // 2, 2 * width)


def on_device(
    inputs, query, key_feat, cotangent, value_weight, output_weight,
    stale_value, stale_output, step_counts, partner,
):
    features = inputs[0]
    upstream_rows = cotangent[0]
    weight_v = value_weight[0]
    weight_o = output_weight[0]
    positions = features.shape[0]
    width = weight_v.shape[1]
    scale_value = D ** (-0.5)
    scale_output = width ** (-0.5)
    rank = lax.axis_index("seq")
    core = rank % 2
    rows_v = weight_v.shape[0]
    rows_o = weight_o.shape[0]

    replicas = lax.axis_size("rep")
    across_v = sent(weight_v, ACROSS)
    twin_v = sent(weight_v, TWIN)
    both_v = sent(across_v, TWIN)
    published = [value_pieces(stale_value[0], replicas), output_pieces(stale_output[0], replicas)]
    spread = swap(jnp.concatenate(published, axis=1))

    twin_features = sent(
        jnp.concatenate(
            [column_block(features, 1 - core, rows_v), column_block(features, 3 - core, rows_v)],
            axis=1,
        ),
        TWIN,
    )
    twin_rows = sent(upstream_rows, TWIN)

    values = None
    for step, block in ((0, weight_v), (1, twin_v), (2, across_v), (3, both_v)):
        part = jnp.dot(
            column_block(features, rank ^ step, rows_v), block, preferred_element_type=f32
        )
        values = part if values is None else values + part
    values = (values * scale_value).astype(bf16)
    query_heads = query[0].reshape(positions, HEADS, HEAD)
    key_heads = key_feat[0].reshape(positions, HEADS, HEAD)
    value_heads = values.reshape(positions, HEADS, HEAD)
    states = jnp.einsum("the,thf->hef", key_heads, value_heads, preferred_element_type=f32)
    states = states.astype(bf16)
    prior = state_sums(states, BEFORE)
    across_oa = sent(weight_o[: rows_o // 2], ACROSS)
    across_ob = sent(weight_o[rows_o // 2 :], ACROSS)
    twin_o = sent(weight_o, TWIN)
    both_oa = sent(across_oa, TWIN)
    both_ob = sent(across_ob, TWIN)
    causal = jnp.arange(positions)[:, None] >= jnp.arange(positions)[None, :]
    scores = jnp.einsum("the,she->hts", query_heads, key_heads, preferred_element_type=f32)
    scores = jnp.where(causal[None], scores, f32(0.0)).astype(bf16)
    attn = jnp.einsum("hts,shf->thf", scores, value_heads, preferred_element_type=f32)
    attn = attn + jnp.einsum("the,hef->thf", query_heads, prior, preferred_element_type=f32)
    inverse = lax.rsqrt(jnp.mean(attn * attn, axis=-1, keepdims=True) + norm_eps)
    unit = attn * inverse
    normed = unit.astype(bf16).reshape(positions, width)

    upstream = jnp.zeros((positions, width), f32)
    for step, start, block in (
        (0, 0, weight_o),
        (1, 0, twin_o),
        (2, 0, across_oa),
        (3, 0, both_oa),
        (2, rows_o // 2, across_ob),
        (3, rows_o // 2, both_ob),
    ):
        part = lax.dot_general(
            upstream_rows, block, (((1,), (1,)), ((), ())), preferred_element_type=f32
        )
        upstream = lax.dynamic_update_slice(upstream, part, (0, (rank ^ step) * rows_o + start))
    upstream = after(upstream, normed)
    upstream = (upstream * scale_output).reshape(positions, HEADS, HEAD)
    d_attn = inverse * (upstream - unit * jnp.mean(unit * upstream, axis=-1, keepdims=True))
    d_attn = d_attn.astype(bf16)
    grad_states = jnp.einsum("the,thf->hef", query_heads, d_attn, preferred_element_type=f32)
    grad_states = grad_states.astype(bf16)
    later = state_sums(grad_states, AFTER)
    d_values = jnp.einsum("hts,thf->shf", scores, d_attn, preferred_element_type=f32)
    d_values = d_values + jnp.einsum("she,hef->shf", key_heads, later, preferred_element_type=f32)
    d_values = d_values.astype(bf16).reshape(positions, width)

    def rows_grad(mine, right, twin, twin_right, width, scale):
        def term(block):
            left = column_block(mine, block, width)
            other = column_block(twin, block // 2, width)
            dims = (((0,), (0,)), ((), ()))
            both = lax.dot_general(left, right, dims, preferred_element_type=f32)
            both += lax.dot_general(other, twin_right, dims, preferred_element_type=f32)
            return both * scale

        away = term(rank ^ 2).astype(bf16)
        back = sent(away, ACROSS)
        return away, back, term(rank)

    twin_normed = sent(
        jnp.concatenate(
            [column_block(normed, 1 - core, rows_o), column_block(normed, 3 - core, rows_o)],
            axis=1,
        ),
        TWIN,
    )
    away_o, back_o, own_o = rows_grad(
        normed, upstream_rows, twin_normed, twin_rows, rows_o, scale_output
    )
    grad_output = own_o + back_o.astype(f32)
    picked = after(spread, grad_states, away_o).at[partner].get(
        mode="promise_in_bounds", unique_indices=True
    )
    fetched = swap(picked)
    _, back_v, grad_value = rows_grad(
        features, d_values, twin_features, sent(d_values, TWIN), rows_v, scale_value
    )
    replica = lax.axis_index("rep")
    own_count = step_counts[replica].astype(f32)
    mate_count = step_counts[partner[replica]].astype(f32)
    mix = mate_count / (own_count + mate_count)
    kept_value = (1.0 - mix) * weight_v.astype(f32) - learning_rate * grad_value
    kept_output = (1.0 - mix) * weight_o.astype(f32) - learning_rate * grad_output
    kept_value, kept_output = lax.optimization_barrier(
        (value_pieces(kept_value, replicas), output_pieces(kept_output, replicas))
    )
    half = kept_value.shape[1]
    back_v = value_pieces(back_v, replicas).astype(f32)
    new_value = kept_value - learning_rate * back_v + mix * fetched[:, :half].astype(f32)
    new_value = new_value.astype(bf16)
    new_output = (kept_output + mix * fetched[:, half:].astype(f32)).astype(bf16)
    return new_value.reshape(value_weight.shape), output_rows(new_output)[None]


def solution(mesh):
    placed = (P("rep", "seq", None),) * 8 + (P(), P())

    return jax.shard_map(
        on_device,
        mesh=mesh,
        in_specs=placed,
        out_specs=(P("rep", "seq", None), P("rep", "seq", None)),
        check_vma=False,
    )
```

```python
import jax
import jax.numpy as jnp
from jax import lax
from jax.sharding import PartitionSpec as P


D = 2048
HEADS = 16
HEAD = 64

learning_rate = 0.25
norm_eps = 1e-06


ACROSS = [(0, 2), (2, 0), (1, 3), (3, 1)]
TWIN = [(0, 1), (1, 0), (2, 3), (3, 2)]
f32 = jnp.float32
bf16 = jnp.bfloat16


def sent(x, pairs):
    return lax.ppermute(x, "seq", pairs)


def column_block(x, block, width):
    return lax.dynamic_slice(x, (0, block * width), (x.shape[0], width))


def state_sums(states, order):
    total = None
    for step in order:
        piece = sent(states, step)
        total = piece.astype(f32) if total is None else total + piece.astype(f32)
    return total.astype(bf16)


BEFORE = ([(0, 1), (2, 3)], [(0, 2), (1, 3)], [(0, 3), (1, 2)])
AFTER = ([(1, 0), (3, 2)], [(2, 0), (3, 1)], [(3, 0), (2, 1)])


def after(x, *others):
    return lax.optimization_barrier((x, *others))[0]


def swap(x):
    return lax.all_to_all(x, "rep", split_axis=0, concat_axis=0, tiled=True)


def value_pieces(x, count):
    return x.reshape(count, x.shape[0] // count, x.shape[1])


def output_pieces(x, count):
    rows, width = 2 * x.shape[0] // count, x.shape[1] // 2
    x = x.reshape(count // 2, rows, 2, width).transpose(0, 2, 1, 3)
    return x.reshape(count, rows, width)


def output_rows(pieces):
    count, rows, width = pieces.shape
    x = pieces.reshape(count // 2, 2, rows, width).transpose(0, 2, 1, 3)
    return x.reshape(count * rows // 2, 2 * width)


def on_device(
    inputs, query, key_feat, cotangent, value_weight, output_weight,
    stale_value, stale_output, step_counts, partner,
):
    features = inputs[0]
    upstream_rows = cotangent[0]
    weight_v = value_weight[0]
    weight_o = output_weight[0]
    positions = features.shape[0]
    width = weight_v.shape[1]
    scale_value = D ** (-0.5)
    scale_output = width ** (-0.5)
    rank = lax.axis_index("seq")
    core = rank % 2
    rows_v = weight_v.shape[0]
    rows_o = weight_o.shape[0]

    replicas = lax.axis_size("rep")
    across_v = sent(weight_v, ACROSS)
    twin_v = sent(weight_v, TWIN)
    both_v = sent(across_v, TWIN)
    published = [value_pieces(stale_value[0], replicas), output_pieces(stale_output[0], replicas)]
    spread = swap(jnp.concatenate(published, axis=1))

    twin_features = sent(
        jnp.concatenate(
            [column_block(features, 1 - core, rows_v), column_block(features, 3 - core, rows_v)],
            axis=1,
        ),
        TWIN,
    )
    twin_rows = sent(upstream_rows, TWIN)

    values = None
    for step, block in ((0, weight_v), (1, twin_v), (2, across_v), (3, both_v)):
        part = jnp.dot(
            column_block(features, rank ^ step, rows_v), block, preferred_element_type=f32
        )
        values = part if values is None else values + part
    values = (values * scale_value).astype(bf16)
    query_heads = query[0].reshape(positions, HEADS, HEAD)
    key_heads = key_feat[0].reshape(positions, HEADS, HEAD)
    value_heads = values.reshape(positions, HEADS, HEAD)
    states = jnp.einsum("the,thf->hef", key_heads, value_heads, preferred_element_type=f32)
    states = states.astype(bf16)
    prior = state_sums(states, BEFORE)
    across_oa = sent(weight_o[: rows_o // 2], ACROSS)
    across_ob = sent(after(weight_o, across_v)[rows_o // 2 :], ACROSS)
    twin_o = sent(weight_o, TWIN)
    both_oa = sent(across_oa, TWIN)
    both_ob = sent(across_ob, TWIN)
    causal = jnp.arange(positions)[:, None] >= jnp.arange(positions)[None, :]
    scores = jnp.einsum("the,she->hts", query_heads, key_heads, preferred_element_type=f32)
    scores = jnp.where(causal[None], scores, f32(0.0)).astype(bf16)
    attn = jnp.einsum("hts,shf->thf", scores, value_heads, preferred_element_type=f32)
    attn = attn + jnp.einsum("the,hef->thf", query_heads, prior, preferred_element_type=f32)
    inverse = lax.rsqrt(jnp.mean(attn * attn, axis=-1, keepdims=True) + norm_eps)
    unit = attn * inverse
    normed = unit.astype(bf16).reshape(positions, width)

    upstream = jnp.zeros((positions, width), f32)
    for step, start, block in (
        (0, 0, weight_o),
        (1, 0, twin_o),
        (2, 0, across_oa),
        (3, 0, both_oa),
        (2, rows_o // 2, across_ob),
        (3, rows_o // 2, both_ob),
    ):
        part = lax.dot_general(
            upstream_rows, block, (((1,), (1,)), ((), ())), preferred_element_type=f32
        )
        column = (rank ^ step) * rows_o + start
        upstream = lax.dynamic_update_slice(upstream, part, (0, column))
    upstream = after(upstream, normed)
    upstream = (upstream * scale_output).reshape(positions, HEADS, HEAD)
    d_attn = inverse * (upstream - unit * jnp.mean(unit * upstream, axis=-1, keepdims=True))
    d_attn = d_attn.astype(bf16)
    grad_states = jnp.einsum("the,thf->hef", query_heads, d_attn, preferred_element_type=f32)
    grad_states = grad_states.astype(bf16)
    later = state_sums(grad_states, AFTER)
    d_values = jnp.einsum("hts,thf->shf", scores, d_attn, preferred_element_type=f32)
    d_values = d_values + jnp.einsum("she,hef->shf", key_heads, later, preferred_element_type=f32)
    d_values = d_values.astype(bf16).reshape(positions, width)

    def rows_grad(mine, right, twin, twin_right, width, scale):
        def term(block):
            left = column_block(mine, block, width)
            other = column_block(twin, block // 2, width)
            dims = (((0,), (0,)), ((), ()))
            both = lax.dot_general(left, right, dims, preferred_element_type=f32)
            both += lax.dot_general(other, twin_right, dims, preferred_element_type=f32)
            return both * scale

        away = term(rank ^ 2).astype(bf16)
        back = sent(away, ACROSS)
        return away, back, term(rank)

    twin_normed = sent(
        jnp.concatenate(
            [column_block(normed, 1 - core, rows_o), column_block(normed, 3 - core, rows_o)],
            axis=1,
        ),
        TWIN,
    )
    away_o, back_o, own_o = rows_grad(
        normed, upstream_rows, twin_normed, twin_rows, rows_o, scale_output
    )
    grad_output = own_o + back_o.astype(f32)
    picked = after(spread, grad_states, away_o).at[partner].get(
        mode="promise_in_bounds", unique_indices=True
    )
    fetched = swap(picked)
    _, back_v, grad_value = rows_grad(
        features, d_values, twin_features, sent(d_values, TWIN), rows_v, scale_value
    )
    replica = lax.axis_index("rep")
    own_count = step_counts[replica].astype(f32)
    mate_count = step_counts[partner[replica]].astype(f32)
    mix = mate_count / (own_count + mate_count)
    kept_value = (1.0 - mix) * weight_v.astype(f32) - learning_rate * grad_value
    kept_output = (1.0 - mix) * weight_o.astype(f32) - learning_rate * grad_output
    kept_value, kept_output = lax.optimization_barrier(
        (value_pieces(kept_value, replicas), output_pieces(kept_output, replicas))
    )
    half = kept_value.shape[1]
    back_v = value_pieces(back_v, replicas).astype(f32)
    new_value = kept_value - learning_rate * back_v + mix * fetched[:, :half].astype(f32)
    new_value = new_value.astype(bf16)
    new_output = (kept_output + mix * fetched[:, half:].astype(f32)).astype(bf16)
    return new_value.reshape(value_weight.shape), output_rows(new_output)[None]


def solution(mesh):
    placed = (P("rep", "seq", None),) * 8 + (P(), P())

    return jax.shard_map(
        on_device,
        mesh=mesh,
        in_specs=placed,
        out_specs=(P("rep", "seq", None), P("rep", "seq", None)),
        check_vma=False,
    )
```

```python
import jax
import jax.numpy as jnp
from jax import lax
from jax.sharding import PartitionSpec as P


D = 2048
HEADS = 16
HEAD = 64

learning_rate = 0.25
norm_eps = 1e-06


ACROSS = [(0, 2), (2, 0), (1, 3), (3, 1)]
TWIN = [(0, 1), (1, 0), (2, 3), (3, 2)]
f32 = jnp.float32
bf16 = jnp.bfloat16


def sent(x, pairs):
    return lax.ppermute(x, "seq", pairs)


def column_block(x, block, width):
    return lax.dynamic_slice(x, (0, block * width), (x.shape[0], width))


def state_sums(states, order):
    total = None
    for step in order:
        piece = sent(states, step)
        total = piece.astype(f32) if total is None else total + piece.astype(f32)
    return total.astype(bf16)


BEFORE = ([(0, 1), (2, 3)], [(0, 2), (1, 3)], [(0, 3), (1, 2)])
AFTER = ([(1, 0), (3, 2)], [(2, 0), (3, 1)], [(3, 0), (2, 1)])


def after(x, *others):
    return lax.optimization_barrier((x, *others))[0]


def swap(x):
    return lax.all_to_all(x, "rep", split_axis=0, concat_axis=0, tiled=True)


def value_pieces(x, count):
    return x.reshape(count, x.shape[0] // count, x.shape[1])


def output_pieces(x, count):
    rows, width = 2 * x.shape[0] // count, x.shape[1] // 2
    x = x.reshape(count // 2, rows, 2, width).transpose(0, 2, 1, 3)
    return x.reshape(count, rows, width)


def output_rows(pieces):
    count, rows, width = pieces.shape
    x = pieces.reshape(count // 2, 2, rows, width).transpose(0, 2, 1, 3)
    return x.reshape(count * rows // 2, 2 * width)


def on_device(
    inputs, query, key_feat, cotangent, value_weight, output_weight,
    stale_value, stale_output, step_counts, partner,
):
    features = inputs[0]
    upstream_rows = cotangent[0]
    weight_v = value_weight[0]
    weight_o = output_weight[0]
    positions = features.shape[0]
    width = weight_v.shape[1]
    scale_value = D ** (-0.5)
    scale_output = width ** (-0.5)
    rank = lax.axis_index("seq")
    core = rank % 2
    rows_v = weight_v.shape[0]
    rows_o = weight_o.shape[0]

    replicas = lax.axis_size("rep")
    across_v = sent(weight_v, ACROSS)
    twin_v = sent(weight_v, TWIN)
    both_v = sent(across_v, TWIN)
    published = [value_pieces(stale_value[0], replicas), output_pieces(stale_output[0], replicas)]
    spread = swap(jnp.concatenate(published, axis=1))

    away_features = jnp.concatenate(
        [column_block(features, 1 - core, rows_v), column_block(features, 3 - core, rows_v)],
        axis=1,
    )
    twin_features = sent(away_features, TWIN)
    twin_rows = sent(upstream_rows, TWIN)

    values = None
    for step, block in ((0, weight_v), (1, twin_v), (2, across_v), (3, both_v)):
        part = jnp.dot(
            column_block(features, rank ^ step, rows_v), block, preferred_element_type=f32
        )
        values = part if values is None else values + part
    values = (values * scale_value).astype(bf16)
    query_heads = query[0].reshape(positions, HEADS, HEAD)
    key_heads = key_feat[0].reshape(positions, HEADS, HEAD)
    value_heads = values.reshape(positions, HEADS, HEAD)
    states = jnp.einsum("the,thf->hef", key_heads, value_heads, preferred_element_type=f32)
    states = states.astype(bf16)
    prior = state_sums(states, BEFORE)
    across_oa = sent(weight_o[: rows_o // 2], ACROSS)
    across_ob = sent(after(weight_o, away_features)[rows_o // 2 :], ACROSS)
    twin_o = sent(weight_o, TWIN)
    both_oa = sent(across_oa, TWIN)
    both_ob = sent(across_ob, TWIN)
    causal = jnp.arange(positions)[:, None] >= jnp.arange(positions)[None, :]
    scores = jnp.einsum("the,she->hts", query_heads, key_heads, preferred_element_type=f32)
    scores = jnp.where(causal[None], scores, f32(0.0)).astype(bf16)
    attn = jnp.einsum("hts,shf->thf", scores, value_heads, preferred_element_type=f32)
    attn = attn + jnp.einsum("the,hef->thf", query_heads, prior, preferred_element_type=f32)
    inverse = lax.rsqrt(jnp.mean(attn * attn, axis=-1, keepdims=True) + norm_eps)
    unit = attn * inverse
    normed = unit.astype(bf16).reshape(positions, width)

    upstream = jnp.zeros((positions, width), f32)
    for step, start, block in (
        (0, 0, weight_o),
        (1, 0, twin_o),
        (2, 0, across_oa),
        (3, 0, both_oa),
        (2, rows_o // 2, across_ob),
        (3, rows_o // 2, both_ob),
    ):
        part = lax.dot_general(
            upstream_rows, block, (((1,), (1,)), ((), ())), preferred_element_type=f32
        )
        column = (rank ^ step) * rows_o + start
        upstream = lax.dynamic_update_slice(upstream, part, (0, column))
    upstream = after(upstream, normed)
    upstream = (upstream * scale_output).reshape(positions, HEADS, HEAD)
    d_attn = inverse * (upstream - unit * jnp.mean(unit * upstream, axis=-1, keepdims=True))
    d_attn = d_attn.astype(bf16)
    grad_states = jnp.einsum("the,thf->hef", query_heads, d_attn, preferred_element_type=f32)
    grad_states = grad_states.astype(bf16)
    later = state_sums(grad_states, AFTER)
    d_values = jnp.einsum("hts,thf->shf", scores, d_attn, preferred_element_type=f32)
    d_values = d_values + jnp.einsum("she,hef->shf", key_heads, later, preferred_element_type=f32)
    d_values = d_values.astype(bf16).reshape(positions, width)

    def rows_grad(mine, right, twin, twin_right, width, scale):
        def term(block):
            left = column_block(mine, block, width)
            other = column_block(twin, block // 2, width)
            dims = (((0,), (0,)), ((), ()))
            both = lax.dot_general(left, right, dims, preferred_element_type=f32)
            both += lax.dot_general(other, twin_right, dims, preferred_element_type=f32)
            return both * scale

        away = term(rank ^ 2).astype(bf16)
        back = sent(away, ACROSS)
        return away, back, term(rank)

    twin_normed = sent(
        jnp.concatenate(
            [column_block(normed, 1 - core, rows_o), column_block(normed, 3 - core, rows_o)],
            axis=1,
        ),
        TWIN,
    )
    away_o, back_o, own_o = rows_grad(
        normed, upstream_rows, twin_normed, twin_rows, rows_o, scale_output
    )
    grad_output = own_o + back_o.astype(f32)
    picked = after(spread, grad_states, away_o).at[partner].get(
        mode="promise_in_bounds", unique_indices=True
    )
    fetched = swap(picked)
    _, back_v, grad_value = rows_grad(
        features, d_values, twin_features, sent(d_values, TWIN), rows_v, scale_value
    )
    replica = lax.axis_index("rep")
    own_count = step_counts[replica].astype(f32)
    mate_count = step_counts[partner[replica]].astype(f32)
    mix = mate_count / (own_count + mate_count)
    kept_value = (1.0 - mix) * weight_v.astype(f32) - learning_rate * grad_value
    kept_output = (1.0 - mix) * weight_o.astype(f32) - learning_rate * grad_output
    kept_value, kept_output = lax.optimization_barrier(
        (value_pieces(kept_value, replicas), output_pieces(kept_output, replicas))
    )
    half = kept_value.shape[1]
    back_v = value_pieces(back_v, replicas).astype(f32)
    new_value = kept_value - learning_rate * back_v + mix * fetched[:, :half].astype(f32)
    new_value = new_value.astype(bf16)
    new_output = (kept_output + mix * fetched[:, half:].astype(f32)).astype(bf16)
    return new_value.reshape(value_weight.shape), output_rows(new_output)[None]


def solution(mesh):
    placed = (P("rep", "seq", None),) * 8 + (P(), P())

    return jax.shard_map(
        on_device,
        mesh=mesh,
        in_specs=placed,
        out_specs=(P("rep", "seq", None), P("rep", "seq", None)),
        check_vma=False,
    )
```
